32 devices in a mesh: freq: 4 (over y, x), pts: 8 (over z, core).
Axes of the slice: x: 2, y: 2, z: 4, core: 2. Of those that a mesh axis runs over, the one named last changes fastest.
Arguments:
- data: float32 [2, 32, 64, 3, 8192], P(None, 'freq', None, None, 'pts'), may hold values from -180 to 180
- quad_weight: float32 [8192], P('pts'), may hold values from 0.2 to 5
- basis: float32 [2, 32, 64, 8], P(None, 'freq'), may hold values from -6 to 6
Outputs:
- basis_out: float32 [2, 32, 64, 8], P(None, 'freq')
- spectrum: float32 [32, 8], P('freq')
- modes: float32 [2, 32, 8, 3, 8192], P(None, 'freq', None, None, 'pts')
The draws below stay inside these ranges and needn't reach their ends.
All inputs are finite; a program needn't handle non-finite values.
Results may differ from the reference program's by a relative error of at most 0.0001.
Values sent between devices are 32-bit elements; how exact they have to be, the bound alone decides.
A program may use at most 128 MiB of HBM per device.

```python
import math
import jax
import jax.numpy as jnp
from jax import lax

BLOCKS = 64
RANK = 8
COMP = 3
ITERS = 4
FREQ_ALL = 32
NPTS = 8192


def draw_data(key, part):
    first, second = jax.random.split(key, 2)
    shape = (2, FREQ_ALL, BLOCKS, COMP, NPTS)
    ramp = 1.0 + 2.0 * jnp.arange(FREQ_ALL, dtype=jnp.float32) / max(FREQ_ALL - 1, 1)
    block_scale = jnp.exp(jax.random.uniform(second, (FREQ_ALL, BLOCKS), jnp.float32, 0.0, math.log(10.0)))
    values = jnp.clip(jax.random.normal(first, shape, jnp.float32), -6.0, 6.0)
    scaled = values * (ramp[:, None] * block_scale)[None, :, :, None, None]
    return scaled.astype(jnp.float32)


def level_of(key, dims, pieces, smallest, high):
    factor_of = 1.0
    for axis_at, parts in pieces:
        heights = jax.random.uniform(jax.random.fold_in(jax.random.fold_in(key, 6), axis_at), (parts,), jnp.float32, smallest / len(pieces), high / len(pieces))
        factor_of = factor_of * jnp.repeat(jnp.exp(heights), dims[axis_at] // parts).reshape((-1,) + (1,) * (len(dims) - 1 - axis_at))
    return factor_of


def scatter_about(stream_key, dims, deviation, limit, shards=(), kind=jnp.bfloat16):
    gain = level_of(stream_key, dims, shards, -0.22, 0.18) if shards else 1.0
    result = jax.random.normal(stream_key, dims, jnp.float32) * deviation * gain
    return jnp.minimum(jnp.maximum(result, -limit), limit).astype(kind)


def setup_inputs(seed: int = 0) -> dict:
    keys = jax.random.split(jax.random.key(seed), 4)
    data = draw_data(jax.random.fold_in(keys[3], 71), 0)
    quad_weight = jnp.clip(jnp.exp(math.log(5.0) - 3.218876 * jax.random.uniform(keys[1], (NPTS,), jnp.float32) ** level_of(keys[1], (NPTS,), ((0, 8),), -0.2, 0.2)), 0.2, 5.0)
    basis = scatter_about(keys[2], (2, FREQ_ALL, BLOCKS, RANK), 1.0, 6.0, ((1, 4),), jnp.float32)
    return dict(data=data, quad_weight=quad_weight, basis=basis)


def matmul_high(left, right):
    return jnp.matmul(left, right, precision=lax.Precision.HIGHEST)

def apply_gram(gram_real, gram_imag, vec_real, vec_imag):
    out_real = matmul_high(gram_real, vec_real) - matmul_high(gram_imag, vec_imag)
    out_imag = matmul_high(gram_real, vec_imag) + matmul_high(gram_imag, vec_real)
    return (out_real, out_imag)

def orthonormalize(z_real, z_imag):
    blocks = z_real.shape[-2]
    cols_real = []
    cols_imag = []
    for column in range(z_real.shape[-1]):
        cur_real = z_real[..., column]
        cur_imag = z_imag[..., column]
        for earlier in range(column):
            base_real = cols_real[earlier]
            base_imag = cols_imag[earlier]
            coef_real = lax.optimization_barrier(jnp.sum(base_real * cur_real + base_imag * cur_imag, axis=-1)) / blocks
            coef_imag = lax.optimization_barrier(jnp.sum(base_real * cur_imag - base_imag * cur_real, axis=-1)) / blocks
            cur_real = cur_real - (coef_real[..., None] * base_real - coef_imag[..., None] * base_imag)
            cur_imag = cur_imag - (coef_real[..., None] * base_imag + coef_imag[..., None] * base_real)
        factor = lax.rsqrt(lax.optimization_barrier(jnp.mean(cur_real * cur_real + cur_imag * cur_imag, axis=-1)) + 1e-06)
        cols_real.append(cur_real * factor[..., None])
        cols_imag.append(cur_imag * factor[..., None])
    return (jnp.stack(cols_real, axis=-1), jnp.stack(cols_imag, axis=-1))

def reference(data, quad_weight, basis):
    scaling = 1.0 / (COMP * NPTS)
    weights = jnp.tile(quad_weight, COMP)

    def one_freq(index):
        block = lax.dynamic_index_in_dim(data, index, 1, keepdims=False)
        samples = block.reshape(2, BLOCKS, COMP * NPTS)
        weighted = samples * weights[None, None, :]
        gram_real = (matmul_high(samples[0], weighted[0].T) + matmul_high(samples[1], weighted[1].T)) * scaling
        gram_imag = (matmul_high(samples[0], weighted[1].T) - matmul_high(samples[1], weighted[0].T)) * scaling
        start = lax.dynamic_index_in_dim(basis, index, 1, keepdims=False)
        vec_real = start[0]
        vec_imag = start[1]
        for step in range(ITERS):
            z_real, z_imag = apply_gram(gram_real, gram_imag, vec_real, vec_imag)
            vec_real, vec_imag = orthonormalize(z_real, z_imag)
        z_real, z_imag = apply_gram(gram_real, gram_imag, vec_real, vec_imag)
        rayleigh = lax.optimization_barrier(jnp.sum(vec_real * z_real + vec_imag * z_imag, axis=-2)) / BLOCKS
        proj_real = matmul_high(vec_real.T, samples[0]) - matmul_high(vec_imag.T, samples[1])
        proj_imag = matmul_high(vec_imag.T, samples[0]) + matmul_high(vec_real.T, samples[1])
        projected = jnp.stack([proj_real, proj_imag]) / BLOCKS
        trace_value = jnp.sum(jnp.diagonal(gram_real))
        return (jnp.stack([vec_real, vec_imag]), rayleigh, projected.reshape(2, RANK, COMP, NPTS), trace_value)
    bases, rayleigh, projected, traces = lax.map(one_freq, jnp.arange(FREQ_ALL, dtype=jnp.int32))
    total = jnp.sum(traces)
    spectrum = rayleigh * (FREQ_ALL * BLOCKS) / total
    return (jnp.moveaxis(bases, 0, 1), spectrum, jnp.moveaxis(projected, 0, 1))
```

```python
import functools

import jax
import jax.numpy as jnp
from jax import lax
from jax.experimental import pallas as pl
from jax.experimental.pallas import tpu as pltpu
from jax.sharding import PartitionSpec as P

ITERS = 4
MESH = pl.DeviceIdType.MESH


def spod_kernel(
    scaling,
    freqs,
    peers,
    groups,
    data_ref,
    weight_ref,
    basis_ref,
    basis_out_ref,
    spectrum_ref,
    modes_ref,
    buf,
    split,
    stage,
    gram_out,
    gram_in,
    trace_out,
    trace_in,
    message,
    load_sem,
    store_sem,
    gram_send,
    gram_recv,
    trace_send,
    trace_recv,
    msg_send,
    msg_recv,
):
    comps, blocks, points = buf.shape[2], buf.shape[3], buf.shape[4]
    rank = basis_ref.shape[2]
    wide = 2 * blocks
    stride = peers // freqs
    me = lax.axis_index("pts")
    row = lax.axis_index("freq")
    mine = me // stride
    is_owner = lax.rem(me, stride) == 0

    def load(f):
        return pltpu.make_async_copy(data_ref.at[:, f], buf.at[f], load_sem.at[f])

    def order(i):
        return lax.rem(mine + 1 + i, freqs)

    for i in range(freqs):
        load(order(i)).start()

    barrier = pltpu.get_barrier_semaphore()
    for step in range(1, peers):
        pl.semaphore_signal(
            barrier, inc=1, device_id={"pts": lax.rem(me + step, peers)}, device_id_type=MESH
        )
    for step in range(1, groups):
        pl.semaphore_signal(
            barrier, inc=1, device_id={"freq": lax.rem(row + step, groups)}, device_id_type=MESH
        )

    root = jnp.sqrt(weight_ref[...])
    inverse = (1.0 / blocks) / root
    lanes = lax.broadcasted_iota(jnp.int32, (1, wide), 1)
    low_minus = jnp.where(lanes < blocks, -1.0, 1.0).astype(jnp.float32)
    high_minus = -low_minus

    def local_gram(f):
        load(f).wait()
        total = jnp.zeros((wide, 2 * wide), jnp.float32)
        for c in range(comps):
            for part in range(2):
                value = buf[f, part, c] * root
                high = value.astype(jnp.bfloat16)
                rest = (value - high.astype(jnp.float32)).astype(jnp.bfloat16)
                split[f, c, part * blocks : (part + 1) * blocks] = high
                split[f, c, wide + part * blocks : wide + (part + 1) * blocks] = rest
            total = total + lax.dot_general(
                split[f, c, :wide],
                split[f, c],
                (((1,), (1,)), ((), ())),
                preferred_element_type=jnp.float32,
            )
        half = 0.5 * total[:, :wide] + total[:, wide:]
        return half[:blocks] + high_minus * pltpu.roll(half[blocks:], blocks, 1)

    def gram_copy(f):
        return pltpu.make_async_remote_copy(
            src_ref=gram_out.at[f],
            dst_ref=gram_in.at[me],
            send_sem=gram_send.at[f],
            recv_sem=gram_recv.at[me],
            device_id={"pts": f * stride},
            device_id_type=MESH,
        )

    first = order(0)
    gram_out[first] = local_gram(first)
    pl.semaphore_wait(barrier, peers - 1 + groups - 1)
    gram_copy(first).start()

    def middle(i, carry):
        f = order(i)
        gram_out[f] = local_gram(f)
        gram_copy(f).start()
        return carry

    lax.fori_loop(1, freqs - 1, middle, 0)
    gram_out[mine] = local_gram(mine)

    if stride > 1:

        @pl.when(jnp.logical_not(is_owner))
        def _():
            gram_copy(mine).start()

    def trace_copy(step):
        return pltpu.make_async_remote_copy(
            src_ref=trace_out,
            dst_ref=trace_in.at[row],
            send_sem=trace_send.at[step],
            recv_sem=trace_recv.at[row],
            device_id={"freq": lax.rem(row + step, groups)},
            device_id_type=MESH,
        )

    def msg_copy(step):
        return pltpu.make_async_remote_copy(
            src_ref=message.at[mine],
            dst_ref=message.at[mine],
            send_sem=msg_send.at[step],
            recv_sem=msg_recv.at[mine],
            device_id={"pts": lax.rem(me + step, peers)},
            device_id_type=MESH,
        )

    @pl.when(is_owner)
    def _():
        def gather(step, total):
            source = lax.rem(me + step, peers)
            pltpu.make_async_copy(gram_in.at[source], gram_in.at[source], gram_recv.at[source]).wait()
            return total + gram_in[source]

        total = lax.fori_loop(1, peers, gather, gram_out[mine]) * scaling
        double = jnp.concatenate([high_minus * total, pltpu.roll(total, blocks, 1)], axis=0)
        matrix = double + double.T
        rows_at = lax.broadcasted_iota(jnp.int32, (wide, wide), 0)
        cols_at = lax.broadcasted_iota(jnp.int32, (wide, wide), 1)
        diagonal = jnp.where(rows_at == cols_at, matrix, 0.0)
        trace = 0.5 * jnp.sum(jnp.sum(diagonal, axis=0, keepdims=True), axis=1, keepdims=True)
        trace_out[...] = jnp.broadcast_to(trace, trace_out.shape)
        for step in range(1, groups):
            trace_copy(step).start()

        def apply(vec):
            return jnp.dot(
                vec, matrix, precision=lax.Precision.HIGHEST, preferred_element_type=jnp.float32
            )

        which = lax.broadcasted_iota(jnp.int32, (rank, wide), 0)

        def step_body(step, vec):
            z = apply(vec)
            turned = low_minus * pltpu.roll(z, blocks, 1)
            for j in range(rank):
                base = z[j : j + 1]
                base_turned = turned[j : j + 1]
                along = jnp.sum(z * base, axis=1, keepdims=True) * (1.0 / blocks)
                across = jnp.sum(z * base_turned, axis=1, keepdims=True) * (1.0 / blocks)
                factor = lax.rsqrt(along[j : j + 1] + 1e-06)
                unit = base * factor
                unit_turned = base_turned * factor
                along = along * factor
                across = across * factor
                z_next = z - (along * unit + across * unit_turned)
                turned_next = turned - (along * unit_turned - across * unit)
                z = jnp.where(which > j, z_next, jnp.where(which == j, unit, z))
                turned = jnp.where(which > j, turned_next, turned)
            return z

        start = jnp.concatenate([basis_ref[0, mine], basis_ref[1, mine]], axis=1)
        vec = lax.fori_loop(0, ITERS, step_body, start)
        energy = jnp.sum(vec * apply(vec), axis=1, keepdims=True) * (1.0 / blocks)
        columns = lax.broadcasted_iota(jnp.int32, (rank, wide), 1)
        energy_row = jnp.sum(jnp.where(which == columns, energy, 0.0), axis=0, keepdims=True)

        group_trace = trace_out[...]
        for step in range(1, groups):
            source = lax.rem(row + step, groups)
            pltpu.make_async_copy(trace_in.at[source], trace_in.at[source], trace_recv.at[source]).wait()
            group_trace = group_trace + trace_in[source]
        message[mine, 0:rank] = vec
        message[mine, rank : rank + 8] = jnp.where(
            lax.broadcasted_iota(jnp.int32, (8, wide), 0) == 0, energy_row, group_trace
        )
        for step in range(1, peers):
            msg_copy(step).start()

    def project(f):
        vec = message[f, 0:rank]
        left = jnp.concatenate([high_minus * vec, pltpu.roll(vec, blocks, 1)], axis=0)
        high = left.astype(jnp.bfloat16)
        rest = (left - high.astype(jnp.float32)).astype(jnp.bfloat16)
        both = jnp.concatenate([high, high], axis=1)
        tail = jnp.concatenate([rest, jnp.zeros_like(rest)], axis=1)
        left = jnp.concatenate([both, tail], axis=0)
        for c in range(comps):
            out = jnp.dot(left, split[f, c], preferred_element_type=jnp.float32)
            out = (out[: 2 * rank] + out[2 * rank :]) * inverse
            stage[f, 0, c] = out[:rank]
            stage[f, 1, c] = out[rank:]
        basis_out_ref[0, f] = vec[:, :blocks]
        basis_out_ref[1, f] = pltpu.roll(vec, blocks, 1)[:, :blocks]
        store(f).start()

    def store(f):
        return pltpu.make_async_copy(stage.at[f], modes_ref.at[:, f], store_sem.at[f])

    def arrive(f):
        pltpu.make_async_copy(message.at[f], message.at[f], msg_recv.at[f]).wait()

    if stride > 1:

        @pl.when(jnp.logical_not(is_owner))
        def _():
            arrive(mine)

    project(mine)

    def others(i, carry):
        f = lax.rem(mine + freqs - i, freqs)
        arrive(f)
        project(f)
        return carry

    lax.fori_loop(1, freqs, others, 0)

    energies = []
    overall = jnp.zeros((1, wide), jnp.float32)
    for f in range(freqs):
        energies.append(message[f, rank : rank + 1])
        overall = overall + message[f, rank + 1 : rank + 2]
    count = freqs * groups * blocks
    spectrum_ref[...] = (jnp.concatenate(energies, axis=0) * count / overall)[:, :rank]

    def finish(i, carry):
        gram_copy(order(i)).wait_send()
        return carry

    lax.fori_loop(0, freqs - 1, finish, 0)
    if stride > 1:

        @pl.when(jnp.logical_not(is_owner))
        def _():
            gram_copy(mine).wait_send()

    @pl.when(is_owner)
    def _():
        for step in range(1, groups):
            trace_copy(step).wait_send()
        for step in range(1, peers):
            msg_copy(step).wait_send()

    for f in range(freqs):
        store(f).wait()


def per_device(peers, groups, data, quad_weight, basis):
    _, freqs, blocks, comps, points = data.shape
    rank = basis.shape[-1]
    assert peers % freqs == 0 and freqs > 2
    scaling = 1.0 / (comps * points * peers)
    wide = 2 * blocks
    vmem = pl.BlockSpec(memory_space=pltpu.VMEM)
    anywhere = pl.BlockSpec(memory_space=pl.ANY)
    f32 = jnp.float32
    basis_t, spectrum, modes_t = pl.pallas_call(
        functools.partial(spod_kernel, scaling, freqs, peers, groups),
        out_shape=(
            jax.ShapeDtypeStruct((2, freqs, rank, blocks), f32),
            jax.ShapeDtypeStruct((freqs, rank), f32),
            jax.ShapeDtypeStruct((2, freqs, comps, rank, points), f32),
        ),
        in_specs=[anywhere, vmem, vmem],
        out_specs=(vmem, vmem, anywhere),
        scratch_shapes=[
            pltpu.VMEM((freqs, 2, comps, blocks, points), f32),
            pltpu.VMEM((freqs, comps, 2 * wide, points), jnp.bfloat16),
            pltpu.VMEM((freqs, 2, comps, rank, points), f32),
            pltpu.VMEM((freqs, blocks, wide), f32),
            pltpu.VMEM((peers, blocks, wide), f32),
            pltpu.VMEM((8, wide), f32),
            pltpu.VMEM((groups, 8, wide), f32),
            pltpu.VMEM((freqs, rank + 8, wide), f32),
            pltpu.SemaphoreType.DMA((freqs,)),
            pltpu.SemaphoreType.DMA((freqs,)),
            pltpu.SemaphoreType.DMA((freqs,)),
            pltpu.SemaphoreType.DMA((peers,)),
            pltpu.SemaphoreType.DMA((groups,)),
            pltpu.SemaphoreType.DMA((groups,)),
            pltpu.SemaphoreType.DMA((peers,)),
            pltpu.SemaphoreType.DMA((freqs,)),
        ],
        compiler_params=pltpu.CompilerParams(
            collective_id=0, has_side_effects=True, vmem_limit_bytes=60 * 1024 * 1024
        ),
        name="spod",
    )(
        data.transpose(0, 1, 3, 2, 4),
        quad_weight.reshape(1, points),
        basis.transpose(0, 1, 3, 2),
    )
    return (
        basis_t.transpose(0, 1, 3, 2),
        spectrum,
        modes_t.transpose(0, 1, 3, 2, 4),
    )


def solution(mesh):
    in_specs = (P(None, "freq", None, None, "pts"), P("pts"), P(None, "freq", None, None))
    out_specs = (P(None, "freq", None, None), P("freq", None), P(None, "freq", None, None, "pts"))
    body = functools.partial(per_device, mesh.shape["pts"], mesh.shape["freq"])
    return jax.shard_map(
        body, mesh=mesh, in_specs=in_specs, out_specs=out_specs, check_vma=False
    )
```

```python
import functools

import jax
import jax.numpy as jnp
from jax import lax
from jax.experimental import pallas as pl
from jax.experimental.pallas import tpu as pltpu
from jax.sharding import PartitionSpec as P

ITERS = 4
MESH = pl.DeviceIdType.MESH


def spod_kernel(
    scaling,
    freqs,
    peers,
    groups,
    data_ref,
    weight_hbm,
    basis_hbm,
    split,
    message_ref,
    inverse_ref,
    buf,
    weight_ref,
    basis_ref,
    small_sem,
    gram_out,
    gram_in,
    trace_out,
    trace_in,
    message,
    load_sem,
    gram_send,
    gram_recv,
    trace_send,
    trace_recv,
    msg_send,
    msg_recv,
):
    comps, blocks, points = buf.shape[2], buf.shape[3], buf.shape[4]
    rank = basis_ref.shape[1]
    wide = 2 * blocks
    stride = peers // freqs
    me = lax.axis_index("pts")
    row = lax.axis_index("freq")
    mine = me // stride
    is_owner = lax.rem(me, stride) == 0

    def load(f):
        return pltpu.make_async_copy(data_ref.at[:, f], buf.at[f], load_sem.at[f])

    def order(i):
        return lax.rem(mine + 1 + i, freqs)

    weight_load = pltpu.make_async_copy(weight_hbm, weight_ref, small_sem.at[0])
    basis_load = pltpu.make_async_copy(basis_hbm.at[:, mine], basis_ref, small_sem.at[1])
    weight_load.start()
    for i in range(freqs):
        load(order(i)).start()
    basis_load.start()

    barrier = pltpu.get_barrier_semaphore()
    for step in range(1, peers):
        pl.semaphore_signal(
            barrier, inc=1, device_id={"pts": lax.rem(me + step, peers)}, device_id_type=MESH
        )
    for step in range(1, groups):
        pl.semaphore_signal(
            barrier, inc=1, device_id={"freq": lax.rem(row + step, groups)}, device_id_type=MESH
        )

    weight_load.wait()
    root = jnp.sqrt(weight_ref[...])
    inverse_ref[...] = (1.0 / blocks) / root
    lanes = lax.broadcasted_iota(jnp.int32, (1, wide), 1)
    low_minus = jnp.where(lanes < blocks, -1.0, 1.0).astype(jnp.float32)
    high_minus = -low_minus

    def local_gram(f):
        load(f).wait()
        total = jnp.zeros((wide, 2 * wide), jnp.float32)
        for c in range(comps):
            for part in range(2):
                value = buf[f, part, c] * root
                high = value.astype(jnp.bfloat16)
                rest = (value - high.astype(jnp.float32)).astype(jnp.bfloat16)
                split[f, c, part * blocks : (part + 1) * blocks] = high
                split[f, c, wide + part * blocks : wide + (part + 1) * blocks] = rest
            total = total + lax.dot_general(
                split[f, c, :wide],
                split[f, c],
                (((1,), (1,)), ((), ())),
                preferred_element_type=jnp.float32,
            )
        half = 0.5 * total[:, :wide] + total[:, wide:]
        return half[:blocks] + high_minus * pltpu.roll(half[blocks:], blocks, 1)

    def gram_copy(f):
        return pltpu.make_async_remote_copy(
            src_ref=gram_out.at[f],
            dst_ref=gram_in.at[me],
            send_sem=gram_send.at[f],
            recv_sem=gram_recv.at[me],
            device_id={"pts": f * stride},
            device_id_type=MESH,
        )

    first = order(0)
    gram_out[first] = local_gram(first)
    pl.semaphore_wait(barrier, peers - 1 + groups - 1)
    gram_copy(first).start()

    def middle(i, carry):
        f = order(i)
        gram_out[f] = local_gram(f)
        gram_copy(f).start()
        return carry

    lax.fori_loop(1, freqs - 1, middle, 0)
    gram_out[mine] = local_gram(mine)

    if stride > 1:

        @pl.when(jnp.logical_not(is_owner))
        def _():
            gram_copy(mine).start()

    def trace_copy(step):
        return pltpu.make_async_remote_copy(
            src_ref=trace_out,
            dst_ref=trace_in.at[row],
            send_sem=trace_send.at[step],
            recv_sem=trace_recv.at[row],
            device_id={"freq": lax.rem(row + step, groups)},
            device_id_type=MESH,
        )

    def msg_copy(step):
        return pltpu.make_async_remote_copy(
            src_ref=message.at[mine],
            dst_ref=message.at[mine],
            send_sem=msg_send.at[step],
            recv_sem=msg_recv.at[mine],
            device_id={"pts": lax.rem(me + step, peers)},
            device_id_type=MESH,
        )

    basis_load.wait()

    @pl.when(is_owner)
    def _():
        def gather(step, total):
            source = lax.rem(me + step, peers)
            pltpu.make_async_copy(gram_in.at[source], gram_in.at[source], gram_recv.at[source]).wait()
            return total + gram_in[source]

        total = lax.fori_loop(1, peers, gather, gram_out[mine]) * scaling
        double = jnp.concatenate([high_minus * total, pltpu.roll(total, blocks, 1)], axis=0)
        matrix = double + double.T
        rows_at = lax.broadcasted_iota(jnp.int32, (wide, wide), 0)
        cols_at = lax.broadcasted_iota(jnp.int32, (wide, wide), 1)
        diagonal = jnp.where(rows_at == cols_at, matrix, 0.0)
        trace = 0.5 * jnp.sum(jnp.sum(diagonal, axis=0, keepdims=True), axis=1, keepdims=True)
        trace_out[...] = jnp.broadcast_to(trace, trace_out.shape)
        for step in range(1, groups):
            trace_copy(step).start()

        def apply(vec):
            return jnp.dot(
                vec, matrix, precision=lax.Precision.HIGHEST, preferred_element_type=jnp.float32
            )

        which = lax.broadcasted_iota(jnp.int32, (rank, wide), 0)

        def step_body(step, vec):
            z = apply(vec)
            turned = low_minus * pltpu.roll(z, blocks, 1)
            for j in range(rank):
                base = z[j : j + 1]
                base_turned = turned[j : j + 1]
                along = jnp.sum(z * base, axis=1, keepdims=True) * (1.0 / blocks)
                across = jnp.sum(z * base_turned, axis=1, keepdims=True) * (1.0 / blocks)
                factor = lax.rsqrt(along[j : j + 1] + 1e-06)
                unit = base * factor
                unit_turned = base_turned * factor
                along = along * factor
                across = across * factor
                z_next = z - (along * unit + across * unit_turned)
                turned_next = turned - (along * unit_turned - across * unit)
                z = jnp.where(which > j, z_next, jnp.where(which == j, unit, z))
                turned = jnp.where(which > j, turned_next, turned)
            return z

        start = jnp.concatenate([basis_ref[0], basis_ref[1]], axis=1)
        vec = lax.fori_loop(0, ITERS, step_body, start)
        energy = jnp.sum(vec * apply(vec), axis=1, keepdims=True) * (1.0 / blocks)
        columns = lax.broadcasted_iota(jnp.int32, (rank, wide), 1)
        energy_row = jnp.sum(jnp.where(which == columns, energy, 0.0), axis=0, keepdims=True)

        group_trace = trace_out[...]
        for step in range(1, groups):
            source = lax.rem(row + step, groups)
            pltpu.make_async_copy(trace_in.at[source], trace_in.at[source], trace_recv.at[source]).wait()
            group_trace = group_trace + trace_in[source]
        message[mine, 0:rank] = vec
        message[mine, rank : rank + 8] = jnp.where(
            lax.broadcasted_iota(jnp.int32, (8, wide), 0) == 0, energy_row, group_trace
        )
        for step in range(1, peers):
            msg_copy(step).start()

    def arrive(f):
        pltpu.make_async_copy(message.at[f], message.at[f], msg_recv.at[f]).wait()

    if stride > 1:

        @pl.when(jnp.logical_not(is_owner))
        def _():
            arrive(mine)

    def others(i, carry):
        arrive(lax.rem(mine + i, freqs))
        return carry

    lax.fori_loop(1, freqs, others, 0)
    message_ref[...] = message[...]

    def finish(i, carry):
        gram_copy(order(i)).wait_send()
        return carry

    lax.fori_loop(0, freqs - 1, finish, 0)
    if stride > 1:

        @pl.when(jnp.logical_not(is_owner))
        def _():
            gram_copy(mine).wait_send()

    @pl.when(is_owner)
    def _():
        for step in range(1, groups):
            trace_copy(step).wait_send()
        for step in range(1, peers):
            msg_copy(step).wait_send()


def project_kernel(
    count, inverse_ref, split, message, basis_out_ref, spectrum_ref, modes_ref, stage, store_sem
):
    freqs, comps, depth, points = split.shape
    wide = depth // 2
    blocks = wide // 2
    rank = spectrum_ref.shape[1]
    inverse = inverse_ref[...]
    lanes = lax.broadcasted_iota(jnp.int32, (1, wide), 1)
    high_minus = jnp.where(lanes < blocks, 1.0, -1.0).astype(jnp.float32)

    def store(f):
        return pltpu.make_async_copy(stage.at[f], modes_ref.at[:, f], store_sem.at[f])

    def project(f, carry):
        vec = message[f, 0:rank]
        left = jnp.concatenate([high_minus * vec, pltpu.roll(vec, blocks, 1)], axis=0)
        high = left.astype(jnp.bfloat16)
        rest = (left - high.astype(jnp.float32)).astype(jnp.bfloat16)
        both = jnp.concatenate([high, high], axis=1)
        tail = jnp.concatenate([rest, jnp.zeros_like(rest)], axis=1)
        left = jnp.concatenate([both, tail], axis=0)
        for c in range(comps):
            out = jnp.dot(left, split[f, c], preferred_element_type=jnp.float32)
            out = (out[: 2 * rank] + out[2 * rank :]) * inverse
            stage[f, 0, c] = out[:rank]
            stage[f, 1, c] = out[rank:]
        store(f).start()
        basis_out_ref[0, f] = vec[:, :blocks]
        basis_out_ref[1, f] = pltpu.roll(vec, blocks, 1)[:, :blocks]
        return carry

    lax.fori_loop(0, freqs, project, 0)

    energies = []
    overall = jnp.zeros((1, wide), jnp.float32)
    for f in range(freqs):
        energies.append(message[f, rank : rank + 1])
        overall = overall + message[f, rank + 1 : rank + 2]
    spectrum_ref[...] = (jnp.concatenate(energies, axis=0) * count / overall)[:, :rank]
    for f in range(freqs):
        store(f).wait()


def per_device(peers, groups, data, quad_weight, basis):
    _, freqs, blocks, comps, points = data.shape
    rank = basis.shape[-1]
    assert peers % freqs == 0 and freqs > 2
    scaling = 1.0 / (comps * points * peers)
    wide = 2 * blocks
    vmem = pl.BlockSpec(memory_space=pltpu.VMEM)
    anywhere = pl.BlockSpec(memory_space=pl.ANY)
    f32 = jnp.float32
    weight = quad_weight.reshape(1, points)
    hbm = pl.BlockSpec(memory_space=pltpu.HBM)
    in_hbm = functools.partial(pltpu.with_memory_space_constraint, memory_space=pltpu.HBM)
    split, message, inverse = pl.pallas_call(
        functools.partial(spod_kernel, scaling, freqs, peers, groups),
        out_shape=(
            pltpu.VMEM((freqs, comps, 2 * wide, points), jnp.bfloat16),
            pltpu.VMEM((freqs, rank + 8, wide), f32),
            pltpu.VMEM((1, points), f32),
        ),
        in_specs=[hbm, hbm, hbm],
        out_specs=(vmem, vmem, vmem),
        scratch_shapes=[
            pltpu.VMEM((freqs, 2, comps, blocks, points), f32),
            pltpu.VMEM((1, points), f32),
            pltpu.VMEM((2, rank, blocks), f32),
            pltpu.SemaphoreType.DMA((2,)),
            pltpu.VMEM((freqs, blocks, wide), f32),
            pltpu.VMEM((peers, blocks, wide), f32),
            pltpu.VMEM((8, wide), f32),
            pltpu.VMEM((groups, 8, wide), f32),
            pltpu.VMEM((freqs, rank + 8, wide), f32),
            pltpu.SemaphoreType.DMA((freqs,)),
            pltpu.SemaphoreType.DMA((freqs,)),
            pltpu.SemaphoreType.DMA((peers,)),
            pltpu.SemaphoreType.DMA((groups,)),
            pltpu.SemaphoreType.DMA((groups,)),
            pltpu.SemaphoreType.DMA((peers,)),
            pltpu.SemaphoreType.DMA((freqs,)),
        ],
        compiler_params=pltpu.CompilerParams(
            collective_id=0, has_side_effects=True, vmem_limit_bytes=40 * 1024 * 1024
        ),
        name="spod",
    )(
        in_hbm(data.transpose(0, 1, 3, 2, 4)),
        in_hbm(weight),
        in_hbm(basis.transpose(0, 1, 3, 2)),
    )
    basis_t, spectrum, modes_t = pl.pallas_call(
        functools.partial(project_kernel, freqs * groups * blocks),
        out_shape=(
            jax.ShapeDtypeStruct((2, freqs, rank, blocks), f32),
            jax.ShapeDtypeStruct((freqs, rank), f32),
            jax.ShapeDtypeStruct((2, freqs, comps, rank, points), f32),
        ),
        in_specs=[vmem, vmem, vmem],
        out_specs=(vmem, vmem, anywhere),
        scratch_shapes=[
            pltpu.VMEM((freqs, 2, comps, rank, points), f32),
            pltpu.SemaphoreType.DMA((freqs,)),
        ],
        compiler_params=pltpu.CompilerParams(vmem_limit_bytes=20 * 1024 * 1024),
        name="project",
    )(inverse, split, message)
    return (
        basis_t.transpose(0, 1, 3, 2),
        spectrum,
        modes_t.transpose(0, 1, 3, 2, 4),
    )


def solution(mesh):
    in_specs = (P(None, "freq", None, None, "pts"), P("pts"), P(None, "freq", None, None))
    out_specs = (P(None, "freq", None, None), P("freq", None), P(None, "freq", None, None, "pts"))
    body = functools.partial(per_device, mesh.shape["pts"], mesh.shape["freq"])
    return jax.shard_map(
        body, mesh=mesh, in_specs=in_specs, out_specs=out_specs, check_vma=False
    )
```

```python
import functools

import jax
import jax.numpy as jnp
from jax import lax
from jax.experimental import pallas as pl
from jax.experimental.pallas import tpu as pltpu
from jax.sharding import PartitionSpec as P

ITERS = 4
MESH = pl.DeviceIdType.MESH


def spod_kernel(
    scaling,
    freqs,
    peers,
    groups,
    data_ref,
    weight_hbm,
    basis_hbm,
    split,
    message_ref,
    inverse_ref,
    buf,
    weight_ref,
    basis_ref,
    small_sem,
    gram_out,
    gram_in,
    trace_out,
    trace_in,
    message,
    load_sem,
    gram_send,
    gram_recv,
    trace_send,
    trace_recv,
    msg_send,
    msg_recv,
):
    comps, blocks, points = buf.shape[2], buf.shape[3], buf.shape[4]
    rank = basis_ref.shape[1]
    wide = 2 * blocks
    stride = peers // freqs
    me = lax.axis_index("pts")
    row = lax.axis_index("freq")
    mine = me // stride
    is_owner = lax.rem(me, stride) == 0

    def load(f):
        return pltpu.make_async_copy(data_ref.at[:, f], buf.at[f], load_sem.at[f])

    def order(i):
        return lax.rem(mine + 1 + i, freqs)

    weight_load = pltpu.make_async_copy(weight_hbm, weight_ref, small_sem.at[0])
    basis_load = pltpu.make_async_copy(basis_hbm.at[:, mine], basis_ref, small_sem.at[1])
    weight_load.start()
    for i in range(freqs):
        load(order(i)).start()
    basis_load.start()

    barrier = pltpu.get_barrier_semaphore()
    for step in range(1, peers):
        pl.semaphore_signal(
            barrier, inc=1, device_id={"pts": lax.rem(me + step, peers)}, device_id_type=MESH
        )
    for step in range(1, groups):
        pl.semaphore_signal(
            barrier, inc=1, device_id={"freq": lax.rem(row + step, groups)}, device_id_type=MESH
        )

    weight_load.wait()
    root = jnp.sqrt(weight_ref[...])
    inverse_ref[...] = (1.0 / blocks) / root
    lanes = lax.broadcasted_iota(jnp.int32, (1, wide), 1)
    low_minus = jnp.where(lanes < blocks, -1.0, 1.0).astype(jnp.float32)
    high_minus = -low_minus

    def local_gram(f):
        load(f).wait()
        total = jnp.zeros((wide, 2 * wide), jnp.float32)
        for c in range(comps):
            for part in range(2):
                value = buf[f, part, c] * root
                high = value.astype(jnp.bfloat16)
                rest = (value - high.astype(jnp.float32)).astype(jnp.bfloat16)
                split[f, c, part * blocks : (part + 1) * blocks] = high
                split[f, c, wide + part * blocks : wide + (part + 1) * blocks] = rest
            total = total + lax.dot_general(
                split[f, c, :wide],
                split[f, c],
                (((1,), (1,)), ((), ())),
                preferred_element_type=jnp.float32,
            )
        half = 0.5 * total[:, :wide] + total[:, wide:]
        return half[:blocks] + high_minus * pltpu.roll(half[blocks:], blocks, 1)

    def gram_copy(f):
        return pltpu.make_async_remote_copy(
            src_ref=gram_out.at[f],
            dst_ref=gram_in.at[me],
            send_sem=gram_send.at[f],
            recv_sem=gram_recv.at[me],
            device_id={"pts": f * stride},
            device_id_type=MESH,
        )

    first = order(0)
    gram_out[first] = local_gram(first)
    pl.semaphore_wait(barrier, peers - 1 + groups - 1)
    gram_copy(first).start()

    def middle(i, carry):
        f = order(i)
        gram_out[f] = local_gram(f)
        gram_copy(f).start()
        return carry

    lax.fori_loop(1, freqs - 1, middle, 0)
    gram_out[mine] = local_gram(mine)

    if stride > 1:

        @pl.when(jnp.logical_not(is_owner))
        def _():
            gram_copy(mine).start()

    def trace_copy(step):
        return pltpu.make_async_remote_copy(
            src_ref=trace_out,
            dst_ref=trace_in.at[row],
            send_sem=trace_send.at[step],
            recv_sem=trace_recv.at[row],
            device_id={"freq": lax.rem(row + step, groups)},
            device_id_type=MESH,
        )

    def msg_copy(step):
        return pltpu.make_async_remote_copy(
            src_ref=message.at[mine],
            dst_ref=message.at[mine],
            send_sem=msg_send.at[step],
            recv_sem=msg_recv.at[mine],
            device_id={"pts": lax.rem(me + step, peers)},
            device_id_type=MESH,
        )

    basis_load.wait()

    @pl.when(is_owner)
    def _():
        def gather(step, total):
            source = lax.rem(me + step, peers)
            pltpu.make_async_copy(gram_in.at[source], gram_in.at[source], gram_recv.at[source]).wait()
            return total + gram_in[source]

        total = lax.fori_loop(1, peers, gather, gram_out[mine]) * scaling
        double = jnp.concatenate([high_minus * total, pltpu.roll(total, blocks, 1)], axis=0)
        matrix = double + double.T
        rows_at = lax.broadcasted_iota(jnp.int32, (wide, wide), 0)
        cols_at = lax.broadcasted_iota(jnp.int32, (wide, wide), 1)
        diagonal = jnp.where(rows_at == cols_at, matrix, 0.0)
        trace = 0.5 * jnp.sum(jnp.sum(diagonal, axis=0, keepdims=True), axis=1, keepdims=True)
        trace_out[...] = jnp.broadcast_to(trace, trace_out.shape)
        for step in range(1, groups):
            trace_copy(step).start()

        def apply(vec):
            return jnp.dot(
                vec, matrix, precision=lax.Precision.HIGHEST, preferred_element_type=jnp.float32
            )

        which = lax.broadcasted_iota(jnp.int32, (rank, wide), 0)

        def step_body(step, vec):
            z = apply(vec)
            turned = low_minus * pltpu.roll(z, blocks, 1)
            for j in range(rank):
                base = z[j : j + 1]
                base_turned = turned[j : j + 1]
                along = jnp.sum(z * base, axis=1, keepdims=True) * (1.0 / blocks)
                across = jnp.sum(z * base_turned, axis=1, keepdims=True) * (1.0 / blocks)
                factor = lax.rsqrt(along[j : j + 1] + 1e-06)
                unit = base * factor
                unit_turned = base_turned * factor
                along = along * factor
                across = across * factor
                z_next = z - (along * unit + across * unit_turned)
                turned_next = turned - (along * unit_turned - across * unit)
                z = jnp.where(which > j, z_next, jnp.where(which == j, unit, z))
                turned = jnp.where(which > j, turned_next, turned)
            return z

        start = jnp.concatenate([basis_ref[0], basis_ref[1]], axis=1)
        vec = lax.fori_loop(0, ITERS, step_body, start)
        energy = jnp.sum(vec * apply(vec), axis=1, keepdims=True) * (1.0 / blocks)
        columns = lax.broadcasted_iota(jnp.int32, (rank, wide), 1)
        energy_row = jnp.sum(jnp.where(which == columns, energy, 0.0), axis=0, keepdims=True)

        group_trace = trace_out[...]
        for step in range(1, groups):
            source = lax.rem(row + step, groups)
            pltpu.make_async_copy(trace_in.at[source], trace_in.at[source], trace_recv.at[source]).wait()
            group_trace = group_trace + trace_in[source]
        message[mine, 0:rank] = vec
        message[mine, rank : rank + 8] = jnp.where(
            lax.broadcasted_iota(jnp.int32, (8, wide), 0) == 0, energy_row, group_trace
        )
        for step in range(1, peers):
            msg_copy(step).start()

    def arrive(f):
        pltpu.make_async_copy(message.at[f], message.at[f], msg_recv.at[f]).wait()

    if stride > 1:

        @pl.when(jnp.logical_not(is_owner))
        def _():
            arrive(mine)

    def others(i, carry):
        arrive(lax.rem(mine + i, freqs))
        return carry

    lax.fori_loop(1, freqs, others, 0)
    message_ref[...] = message[...]

    def finish(i, carry):
        gram_copy(order(i)).wait_send()
        return carry

    lax.fori_loop(0, freqs - 1, finish, 0)
    if stride > 1:

        @pl.when(jnp.logical_not(is_owner))
        def _():
            gram_copy(mine).wait_send()

    @pl.when(is_owner)
    def _():
        for step in range(1, groups):
            trace_copy(step).wait_send()
        for step in range(1, peers):
            msg_copy(step).wait_send()


def project_kernel(
    count, inverse_ref, split, message, basis_out_ref, spectrum_ref, modes_ref, stage, store_sem
):
    freqs, comps, depth, points = split.shape
    wide = depth // 2
    blocks = wide // 2
    rank = spectrum_ref.shape[1]
    inverse = inverse_ref[...]
    lanes = lax.broadcasted_iota(jnp.int32, (1, wide), 1)
    high_minus = jnp.where(lanes < blocks, 1.0, -1.0).astype(jnp.float32)

    def store(f):
        return pltpu.make_async_copy(stage.at[f], modes_ref.at[:, f], store_sem.at[f])

    def project(f, carry):
        vec = message[f, 0:rank]
        left = jnp.concatenate([high_minus * vec, pltpu.roll(vec, blocks, 1)], axis=0)
        high = left.astype(jnp.bfloat16)
        rest = (left - high.astype(jnp.float32)).astype(jnp.bfloat16)
        both = jnp.concatenate([high, high], axis=1)
        tail = jnp.concatenate([rest, jnp.zeros_like(rest)], axis=1)
        left = jnp.concatenate([both, tail], axis=0)
        for c in range(comps):
            out = jnp.dot(left, split[f, c], preferred_element_type=jnp.float32)
            out = (out[: 2 * rank] + out[2 * rank :]) * inverse
            stage[f, 0, c] = out[:rank]
            stage[f, 1, c] = out[rank:]
        store(f).start()
        basis_out_ref[0, f] = vec[:, :blocks]
        basis_out_ref[1, f] = pltpu.roll(vec, blocks, 1)[:, :blocks]
        return carry

    lax.fori_loop(0, freqs, project, 0, unroll=True)

    energies = []
    overall = jnp.zeros((1, wide), jnp.float32)
    for f in range(freqs):
        energies.append(message[f, rank : rank + 1])
        overall = overall + message[f, rank + 1 : rank + 2]
    spectrum_ref[...] = (jnp.concatenate(energies, axis=0) * count / overall)[:, :rank]
    for f in range(freqs):
        store(f).wait()


def per_device(peers, groups, data, quad_weight, basis):
    _, freqs, blocks, comps, points = data.shape
    rank = basis.shape[-1]
    assert peers % freqs == 0 and freqs > 2
    scaling = 1.0 / (comps * points * peers)
    wide = 2 * blocks
    vmem = pl.BlockSpec(memory_space=pltpu.VMEM)
    anywhere = pl.BlockSpec(memory_space=pl.ANY)
    f32 = jnp.float32
    weight = quad_weight.reshape(1, points)
    hbm = pl.BlockSpec(memory_space=pltpu.HBM)
    in_hbm = functools.partial(pltpu.with_memory_space_constraint, memory_space=pltpu.HBM)
    split, message, inverse = pl.pallas_call(
        functools.partial(spod_kernel, scaling, freqs, peers, groups),
        out_shape=(
            pltpu.VMEM((freqs, comps, 2 * wide, points), jnp.bfloat16),
            pltpu.VMEM((freqs, rank + 8, wide), f32),
            pltpu.VMEM((1, points), f32),
        ),
        in_specs=[hbm, hbm, hbm],
        out_specs=(vmem, vmem, vmem),
        scratch_shapes=[
            pltpu.VMEM((freqs, 2, comps, blocks, points), f32),
            pltpu.VMEM((1, points), f32),
            pltpu.VMEM((2, rank, blocks), f32),
            pltpu.SemaphoreType.DMA((2,)),
            pltpu.VMEM((freqs, blocks, wide), f32),
            pltpu.VMEM((peers, blocks, wide), f32),
            pltpu.VMEM((8, wide), f32),
            pltpu.VMEM((groups, 8, wide), f32),
            pltpu.VMEM((freqs, rank + 8, wide), f32),
            pltpu.SemaphoreType.DMA((freqs,)),
            pltpu.SemaphoreType.DMA((freqs,)),
            pltpu.SemaphoreType.DMA((peers,)),
            pltpu.SemaphoreType.DMA((groups,)),
            pltpu.SemaphoreType.DMA((groups,)),
            pltpu.SemaphoreType.DMA((peers,)),
            pltpu.SemaphoreType.DMA((freqs,)),
        ],
        compiler_params=pltpu.CompilerParams(
            collective_id=0, has_side_effects=True, vmem_limit_bytes=40 * 1024 * 1024
        ),
        name="spod",
    )(
        in_hbm(data.transpose(0, 1, 3, 2, 4)),
        in_hbm(weight),
        in_hbm(basis.transpose(0, 1, 3, 2)),
    )
    basis_t, spectrum, modes_t = pl.pallas_call(
        functools.partial(project_kernel, freqs * groups * blocks),
        out_shape=(
            jax.ShapeDtypeStruct((2, freqs, rank, blocks), f32),
            jax.ShapeDtypeStruct((freqs, rank), f32),
            jax.ShapeDtypeStruct((2, freqs, comps, rank, points), f32),
        ),
        in_specs=[vmem, vmem, vmem],
        out_specs=(vmem, vmem, anywhere),
        scratch_shapes=[
            pltpu.VMEM((freqs, 2, comps, rank, points), f32),
            pltpu.SemaphoreType.DMA((freqs,)),
        ],
        compiler_params=pltpu.CompilerParams(vmem_limit_bytes=20 * 1024 * 1024),
        name="project",
    )(inverse, split, message)
    return (
        basis_t.transpose(0, 1, 3, 2),
        spectrum,
        modes_t.transpose(0, 1, 3, 2, 4),
    )


def solution(mesh):
    in_specs = (P(None, "freq", None, None, "pts"), P("pts"), P(None, "freq", None, None))
    out_specs = (P(None, "freq", None, None), P("freq", None), P(None, "freq", None, None, "pts"))
    body = functools.partial(per_device, mesh.shape["pts"], mesh.shape["freq"])
    return jax.shard_map(
        body, mesh=mesh, in_specs=in_specs, out_specs=out_specs, check_vma=False
    )
```
